32 devices in a mesh: blk: 16 (over z, x, core), cuts: 2 (over y).
Axes of the slice: x: 2, y: 2, z: 4, core: 2. Of those that a mesh axis runs over, the one named last changes fastest.
Arguments:
- left_env: bfloat16 [2048, 8, 2048], P('blk', 'cuts'), may hold values from -4 to 4
- right_env: bfloat16 [2048, 8, 2048], P('blk', 'cuts'), may hold values from -4 to 4
- left_core: float32 [8, 8, 2, 2], replicated, may hold values from -1.5 to 1.5
- right_core: float32 [8, 8, 2, 2], replicated, may hold values from -1.5 to 1.5
- slot_bond: int32 [8], replicated, may hold values from 0 to 7, each once
- krylov_basis: float32 [8, 2048, 4, 2048], P(None, 'blk', None, 'cuts'), may hold values from -30 to 30
- beta_prev: float32 [], replicated, may hold values from 0.3 to 1.2
Outputs:
- next_vector: float32 [2048, 4, 2048], P('blk', None, 'cuts')
- alpha_values: float32 [1], replicated
- beta_values: float32 [1], replicated
The draws below stay inside these ranges and needn't reach their ends.
Inputs may be any that keep to these rules, and one draw needn't show every extreme that they name: `slot_bond`: a permutation of the 8 bond values.
All inputs are finite; a program needn't handle non-finite values.
Results may differ from the reference program's by a relative error of at most 0.00073.
The reference program's roundings to bfloat16 on the way (of `current` and `mixed_left`) count: a program that leaves them out, or rounds other values in their place, can miss the bound.
Values may be sent and summed in bfloat16 or wider, within the bound.
No kernel may reach another device: no remote copies, remote signals or barrier semaphores. Data moves between devices by JAX's collectives and lax.ppermute only.
A program may use at most 192 MiB of HBM per device.

```python
import math
import jax
import jax.numpy as jnp
from jax import lax

D = 2048
PHYS = 2
W = 8
KRY = 8
STEPS = 1


def draw_environment(key):
    key_noise, key_diag = jax.random.split(key, 2)
    noise_part = jnp.clip(jax.random.normal(key_noise, (D, W, D), jnp.float32), -6.0, 6.0) * (0.8 / math.sqrt(D))
    diag_values = jax.random.uniform(key_diag, (D, W), jnp.float32, 0.5, 1.5)
    on_diagonal = jnp.arange(D, dtype=jnp.int32)[:, None, None] == jnp.arange(D, dtype=jnp.int32)[None, None, :]
    return (noise_part + jnp.where(on_diagonal, diag_values[:, :, None], 0.0)).astype(jnp.bfloat16)


def draw_left_env(key, part):
    return draw_environment(jax.random.fold_in(key, 11))


def draw_right_env(key, part):
    return draw_environment(jax.random.fold_in(key, 23))


def draw_krylov_basis(key, part):
    key_common, key_single = jax.random.split(jax.random.fold_in(key, 37), 2)
    one_shape = (D, PHYS * PHYS, D)
    rising_scale = jnp.exp(math.log(3.0) * jnp.arange(D, dtype=jnp.float32) / D)[:, None, None]
    common = jnp.clip(jax.random.normal(key_common, one_shape, jnp.float32), -6.0, 6.0)
    single = jnp.clip(jax.random.normal(key_single, (KRY,) + one_shape, jnp.float32), -6.0, 6.0)
    return rising_scale[None] * (0.6 * common[None] + 0.8 * single)


def bell_draw(own_key, shape, scale, bound, kind=jnp.bfloat16):
    values = scale * jax.random.normal(own_key, shape, jnp.float32)
    return jnp.clip(values, min=-bound, max=bound).astype(kind)


def setup_inputs(seed: int = 0) -> dict:
    streams_of = jax.random.split(jax.random.key(seed), 8)
    left_env = draw_left_env(jax.random.fold_in(streams_of[7], 71), 0)
    right_env = draw_right_env(jax.random.fold_in(streams_of[7], 71), 0)
    left_core = bell_draw(streams_of[2], (W, W, PHYS, PHYS), (W * PHYS) ** -0.5, 1.5, jnp.float32)
    right_core = bell_draw(streams_of[3], (W, W, PHYS, PHYS), (W * PHYS) ** -0.5, 1.5, jnp.float32)
    slot_bond = jax.random.permutation(streams_of[4], W).astype(jnp.int32)
    krylov_basis = draw_krylov_basis(jax.random.fold_in(streams_of[7], 71), 0)
    beta_prev = jnp.clip(jax.random.uniform(streams_of[6], (), jnp.float32, 0.3, 1.2), 0.3, 1.2)
    return dict(left_env=left_env, right_env=right_env, left_core=left_core, right_core=right_core, slot_bond=slot_bond, krylov_basis=krylov_basis, beta_prev=beta_prev)


def build_table(left_core, right_core, slot_bond):
    picked = left_core[slot_bond]
    table = jnp.einsum('kxac,xybd->kyabcd', picked, right_core, precision=lax.Precision.HIGHEST)
    return table.reshape(W, W, PHYS * PHYS, PHYS * PHYS)

def apply_hamiltonian(left_env, right_env, mpo_table, current):
    pair_count = PHYS * PHYS
    block_rows = min(D, 256)
    block_count = D // block_rows
    right_matrix = right_env.reshape(D, W * D).T
    vector_matrix = current.reshape(D, pair_count * D)

    def one_block(block_index):
        start_row = (block_index * block_rows).astype(jnp.int32)
        left_rows = lax.dynamic_slice_in_dim(left_env, start_row, block_rows, 0).reshape(block_rows * W, D)
        projected = jnp.dot(left_rows, vector_matrix, preferred_element_type=jnp.float32)
        projected = projected.reshape(block_rows, W, pair_count, D)
        mixed_left = jnp.einsum('kypq,akqb->apyb', mpo_table, projected, precision=lax.Precision.HIGHEST).astype(jnp.bfloat16)
        image_rows = jnp.dot(mixed_left.reshape(block_rows * pair_count, W * D), right_matrix, preferred_element_type=jnp.float32)
        return image_rows.reshape(block_rows, pair_count, D)
    image_vec = lax.map(one_block, jnp.arange(block_count, dtype=jnp.int32))
    return image_vec.reshape(D, pair_count, D)

def reference(left_env, right_env, left_core, right_core, slot_bond, krylov_basis, beta_prev):
    highest = lax.Precision.HIGHEST
    entries = float(D * PHYS * PHYS * D)
    mpo_table = build_table(left_core, right_core, slot_bond)
    basis_now = krylov_basis
    beta_now = beta_prev
    alpha_list = []
    beta_list = []
    next_vector = krylov_basis[KRY - 1]
    for step_index in range(STEPS):
        current_f = basis_now[KRY - 1]
        previous = basis_now[KRY - 2]
        image_vec = apply_hamiltonian(left_env, right_env, mpo_table, current_f.astype(jnp.bfloat16))
        alpha_now = jnp.sum(current_f * image_vec) / entries
        first_pass = image_vec - alpha_now * current_f - beta_now * previous
        ortho_coeffs = jnp.einsum('japb,apb->j', basis_now, first_pass, precision=highest) / entries
        second_pass = first_pass - jnp.einsum('j,japb->apb', ortho_coeffs, basis_now, precision=highest)
        beta_new = jnp.sqrt(jnp.sum(second_pass * second_pass) / entries + 1e-06)
        next_vector = second_pass / beta_new
        alpha_list.append(alpha_now)
        beta_list.append(beta_new)
        basis_now = jnp.concatenate([basis_now[1:], next_vector[None]], axis=0)
        beta_now = beta_new
    return (next_vector, jnp.stack(alpha_list), jnp.stack(beta_list))
```

```python
import jax
import jax.numpy as jnp
from jax import lax
from jax.sharding import PartitionSpec as P


def build_table(left_core, right_core, slot_bond):
    bond_width = left_core.shape[0]
    phys_dim = left_core.shape[2]
    chosen = (slot_bond[:, None] == jnp.arange(bond_width, dtype=jnp.int32)[None, :]).astype(
        jnp.float32
    )
    picked = jnp.einsum("kw,wxac->kxac", chosen, left_core, precision=lax.Precision.HIGHEST)
    table = jnp.einsum("kxac,xybd->kyabcd", picked, right_core, precision=lax.Precision.HIGHEST)
    return table.reshape(bond_width, bond_width, phys_dim * phys_dim, phys_dim * phys_dim)


def on_device(left_env, right_env, left_core, right_core, slot_bond, krylov_basis, beta_prev):
    highest = lax.Precision.HIGHEST
    bond_width = left_core.shape[0]
    pair_count = left_core.shape[2] * left_core.shape[2]
    basis_count = krylov_basis.shape[0]
    row_count = krylov_basis.shape[1]
    col_count = krylov_basis.shape[3]
    full_width = left_env.shape[2]
    entries = float(full_width * pair_count * full_width)
    mpo_table = build_table(left_core, right_core, slot_bond)
    cut_count = lax.axis_size("cuts")
    cut_index = lax.axis_index("cuts")
    paired = cut_count == 2
    swap = [(0, 1), (1, 0)]
    current_f = krylov_basis[basis_count - 1]
    current = current_f.astype(jnp.bfloat16)
    block_rows = lax.all_gather(current, "blk", axis=0, tiled=True)
    if paired:
        half = left_env.shape[1]
        left_full = jnp.concatenate([left_env, lax.ppermute(left_env, "cuts", swap)], axis=1)
        kept = lax.dynamic_slice_in_dim(right_env, cut_index * col_count, col_count, 2)
        sent = lax.dynamic_slice_in_dim(right_env, (1 - cut_index) * col_count, col_count, 2)
        right_local = jnp.concatenate([kept, lax.ppermute(sent, "cuts", swap)], axis=1)
        turned = jnp.roll(mpo_table, (half, half), axis=(0, 1))
        mpo_table = jnp.where(cut_index == 0, mpo_table, turned)
    else:
        left_full = lax.all_gather(left_env, "cuts", axis=1, tiled=True)
        right_local = lax.all_to_all(right_env, "cuts", split_axis=2, concat_axis=1, tiled=True)
    local_gram = jnp.einsum("japb,kapb->jk", krylov_basis, krylov_basis, precision=highest)
    right_rows = right_local.shape[0]
    chunk_count = 2 if paired and right_rows % 32 == 0 else 1
    chunk_rows = right_rows // chunk_count
    chunks = [
        right_local[index * chunk_rows : (index + 1) * chunk_rows] for index in range(chunk_count)
    ]
    chunks, block_rows, left_full, local_gram = lax.optimization_barrier(
        (chunks, block_rows, left_full, local_gram)
    )
    gathered = [lax.all_gather(chunk, "blk", axis=0, tiled=True) for chunk in chunks]
    left_matrix = left_full.reshape(row_count * bond_width, full_width)
    projected = jnp.dot(
        left_matrix,
        block_rows.reshape(block_rows.shape[0], pair_count * col_count),
        preferred_element_type=jnp.float32,
    )
    projected = projected.reshape(row_count, bond_width, pair_count, col_count)
    mixed_left = jnp.einsum("kypq,akqb->apyb", mpo_table, projected, precision=highest).astype(
        jnp.bfloat16
    )
    left_side = mixed_left.reshape(row_count * pair_count, bond_width * col_count)
    pieces = []
    for rows in gathered:
        partial_terms = lax.dot_general(
            left_side,
            rows.reshape(rows.shape[0], -1),
            (((1,), (1,)), ((), ())),
            preferred_element_type=jnp.float32,
        )
        width = partial_terms.shape[1] // cut_count
        partial_terms = partial_terms.reshape(row_count, pair_count, cut_count * width)
        if paired:
            own = lax.dynamic_slice_in_dim(partial_terms, cut_index * width, width, 2)
            other = lax.dynamic_slice_in_dim(partial_terms, (1 - cut_index) * width, width, 2)
            piece = own + lax.ppermute(other, "cuts", swap)
        else:
            piece = lax.psum_scatter(partial_terms, "cuts", scatter_dimension=2, tiled=True)
        pieces.append(piece.reshape(row_count, pair_count, width // chunk_rows, chunk_rows))
    image_vec = jnp.concatenate(pieces, axis=3).reshape(row_count, pair_count, col_count)
    local_prods = jnp.sum(krylov_basis * image_vec[None], axis=(1, 2, 3))
    gram_matrix, inner_prods, image_square = lax.psum(
        (local_gram, local_prods, jnp.sum(image_vec * image_vec)), ("blk", "cuts")
    )
    gram_matrix = gram_matrix / entries
    inner_prods = inner_prods / entries
    image_square = image_square / entries
    alpha_now = inner_prods[basis_count - 1]
    ortho_coeffs = (
        inner_prods
        - alpha_now * gram_matrix[:, basis_count - 1]
        - beta_prev * gram_matrix[:, basis_count - 2]
    )
    first_square = (
        image_square
        - 2.0 * alpha_now * inner_prods[basis_count - 1]
        - 2.0 * beta_prev * inner_prods[basis_count - 2]
        + alpha_now * alpha_now * gram_matrix[basis_count - 1, basis_count - 1]
        + 2.0 * alpha_now * beta_prev * gram_matrix[basis_count - 1, basis_count - 2]
        + beta_prev * beta_prev * gram_matrix[basis_count - 2, basis_count - 2]
    )
    square_mean = (
        first_square
        - 2.0 * jnp.sum(ortho_coeffs * ortho_coeffs)
        + jnp.sum(ortho_coeffs[:, None] * gram_matrix * ortho_coeffs[None, :])
    )
    beta_new = jnp.sqrt(square_mean + 1e-06)
    weights = ortho_coeffs.at[basis_count - 1].add(alpha_now).at[basis_count - 2].add(beta_prev)
    removed = weights[0] * krylov_basis[0]
    for index in range(1, basis_count):
        removed = removed + weights[index] * krylov_basis[index]
    next_vector = (image_vec - removed) / beta_new
    alpha_list = [alpha_now]
    beta_list = [beta_new]
    return (next_vector, jnp.stack(alpha_list), jnp.stack(beta_list))


def solution(mesh):
    in_specs = (
        P("blk", "cuts", None),
        P("blk", "cuts", None),
        P(),
        P(),
        P(),
        P(None, "blk", None, "cuts"),
        P(),
    )
    out_specs = (P("blk", None, "cuts"), P(), P())
    return jax.shard_map(
        on_device, mesh=mesh, in_specs=in_specs, out_specs=out_specs, check_vma=False
    )
```
